32 devices in a mesh: dp: 16 (over z, x, core), tensor: 2 (over y).
Axes of the slice: x: 2, y: 2, z: 4, core: 2. Of those that a mesh axis runs over, the one named last changes fastest.
Arguments:
- tokens: bfloat16 [8192, 1152], P(('dp', 'tensor')), may hold values from -6 to 6
- condition: bfloat16 [32, 1152], P(('dp', 'tensor')), may hold values from -6 to 6
- w_qkv: bfloat16 [1152, 3, 1152], P('dp', None, 'tensor'), may hold values from -0.1875 to 0.1875
- qv_bias: bfloat16 [2, 1152], P(None, 'tensor'), may hold values from -3 to 3
- w_proj: bfloat16 [1152, 1152], P('tensor', 'dp'), may hold values from -1 to 1
- proj_bias: bfloat16 [1152], replicated, may hold values from -3 to 3
- w_fc1: bfloat16 [1152, 4608], P('dp', 'tensor'), may hold values from -0.1875 to 0.1875
- fc1_bias: bfloat16 [4608], P('tensor'), may hold values from -3 to 3
- w_fc2: bfloat16 [4608, 1152], P('tensor', 'dp'), may hold values from -0.09375 to 0.09375
- fc2_bias: bfloat16 [1152], replicated, may hold values from -3 to 3
- w_ada: bfloat16 [1152, 6912], P(None, ('dp', 'tensor')), may hold values from -0.1875 to 0.1875
- ada_bias: bfloat16 [6912], P(('dp', 'tensor')), may hold values from -3 to 3
- cotangent: bfloat16 [8192, 1152], P(('dp', 'tensor')), may hold values from -6 to 6
Outputs:
- output: bfloat16 [8192, 1152], P(('dp', 'tensor'))
- grad_tokens: float32 [8192, 1152], P(('dp', 'tensor'))
- grad_condition: float32 [32, 1152], P(('dp', 'tensor'))
- grad_w_qkv: float32 [1152, 3, 1152], P('dp', None, 'tensor')
- grad_qv_bias: float32 [2, 1152], P(None, 'tensor')
- grad_w_proj: float32 [1152, 1152], P('tensor', 'dp')
- grad_proj_bias: float32 [1152], replicated
- grad_w_fc1: float32 [1152, 4608], P('dp', 'tensor')
- grad_fc1_bias: float32 [4608], P('tensor')
- grad_w_fc2: float32 [4608, 1152], P('tensor', 'dp')
- grad_fc2_bias: float32 [1152], replicated
- grad_w_ada: float32 [1152, 6912], P(None, ('dp', 'tensor'))
- grad_ada_bias: float32 [6912], P(('dp', 'tensor'))
The draws below stay inside these ranges and needn't reach their ends.
All inputs are finite; a program needn't handle non-finite values.
Results may differ from the reference program's by a relative error of at most 0.015.
The reference program's roundings to bfloat16 on the way count: a program that leaves them out, or rounds other values in their place, can miss the bound.
Values may be sent and summed in bfloat16 or wider, within the bound.
A program may use at most 128 MiB of HBM per device.

```python
import jax
import jax.numpy as jnp
from jax import lax

D = 1152
HEADS = 16
HEAD_DIM = 72
FF = 4608
L = 256
SEQ_DEV = 2
SEQS = 32
TOKENS = 8192


def steps_of(stream_key, shape, split, smallest, top_value):
    level, own = 1.0, jax.random.fold_in(stream_key, 6)
    for axis_at, parts in split:
        steps = jnp.exp(jax.random.uniform(jax.random.fold_in(own, axis_at), (parts,), jnp.float32, smallest / len(split), top_value / len(split)))
        level = level * jnp.repeat(steps, shape[axis_at] // parts).reshape([-1 if axis == axis_at else 1 for axis in range(len(shape))])
    return level


def scatter_about(rng, dims, spread, reach, shards=(), dtype=jnp.bfloat16):
    loudness = steps_of(rng, dims, shards, -0.22, 0.18) if shards else 1.0
    array = jax.random.normal(rng, dims, jnp.float32) * spread * loudness
    return jnp.minimum(jnp.maximum(array, -reach), reach).astype(dtype)


def setup_inputs(seed: int = 0) -> dict:
    key_list = jax.random.split(jax.random.key(seed), 14)
    tokens = scatter_about(key_list[0], (TOKENS, D), 1.0, 6.0, ((0, 32),))
    condition = scatter_about(key_list[1], (SEQS, D), 1.0, 6.0, ((0, 32),))
    w_qkv = scatter_about(key_list[2], (D, 3, D), D ** -0.5, 0.1875, ((0, 16), (2, 2)))
    qv_bias = scatter_about(key_list[3], (2, D), 0.5, 3.0, ((1, 2),))
    w_proj = scatter_about(key_list[4], (D, D), (D // 32) ** -0.5, 1.0, ((0, 2), (1, 16)))
    proj_bias = scatter_about(key_list[5], (D,), 0.5, 3.0)
    w_fc1 = scatter_about(key_list[6], (D, FF), D ** -0.5, 0.1875, ((0, 16), (1, 2)))
    fc1_bias = scatter_about(key_list[7], (FF,), 0.5, 3.0, ((0, 2),))
    w_fc2 = scatter_about(key_list[8], (FF, D), FF ** -0.5, 0.09375, ((0, 2), (1, 16)))
    fc2_bias = scatter_about(key_list[9], (D,), 0.5, 3.0)
    w_ada = scatter_about(key_list[10], (D, 6 * D), D ** -0.5, 0.1875, ((1, 32),))
    ada_bias = scatter_about(key_list[11], (6 * D,), 0.5, 3.0, ((0, 32),))
    cotangent = scatter_about(key_list[12], (TOKENS, D), 1.0, 6.0, ((0, 32),))
    return dict(tokens=tokens, condition=condition, w_qkv=w_qkv, qv_bias=qv_bias, w_proj=w_proj, proj_bias=proj_bias, w_fc1=w_fc1, fc1_bias=fc1_bias, w_fc2=w_fc2, fc2_bias=fc2_bias, w_ada=w_ada, ada_bias=ada_bias, cotangent=cotangent)


@jax.custom_vjp
def low(v):
    return lax.optimization_barrier(v.astype(jnp.bfloat16)).astype(jnp.float32)

@jax.custom_vjp
def low_back(v):
    return v

def low_keep(v):
    return (low(v), None)

def low_pass(kept, grad):
    return (grad,)

def back_keep(v):
    return (v, None)

def back_low(kept, grad):
    return (low(grad),)
low.defvjp(low_keep, low_pass)
low_back.defvjp(back_keep, back_low)
eps = 1e-06
highest = lax.Precision.HIGHEST

def layer_norm(values):
    center = values - lax.optimization_barrier(jnp.mean(values, axis=-1, keepdims=True))
    return center * lax.rsqrt(lax.optimization_barrier(jnp.mean(center * center, axis=-1, keepdims=True)) + eps)

def forward(block_tokens, block_cond, w_qkv, qv_bias, w_proj, proj_bias, w_fc1, fc1_bias, w_fc2, fc2_bias, w_ada, ada_bias):
    latents = block_cond.shape[0]
    modulation = jnp.dot(low(jax.nn.silu(block_cond)), w_ada, precision=highest) + ada_bias
    modulation = low(low_back(modulation)).reshape(latents, 6, 1, D)
    residual = block_tokens.reshape(latents, L, D)
    attn_input = low(layer_norm(residual) * (1.0 + modulation[:, 1]) + modulation[:, 0]).reshape(latents * L, D)
    projected = jnp.einsum('td,dkf->tkf', attn_input, w_qkv, precision=highest)
    head_shape = (latents, L, HEADS, HEAD_DIM)
    queries = low(low_back(projected[:, 0] + qv_bias[0])).reshape(head_shape)
    key_all = low(low_back(projected[:, 1])).reshape(head_shape)
    value_all = low(low_back(projected[:, 2] + qv_bias[1])).reshape(head_shape)
    scores = low_back(jnp.einsum('sqhe,skhe->shqk', queries, key_all, precision=highest) * HEAD_DIM ** (-0.5))
    probs = low(jax.nn.softmax(scores, axis=-1))
    mixed = jnp.einsum('shqk,skhe->sqhe', probs, value_all, precision=highest).reshape(latents * L, D)
    mixed = low(low_back(mixed))
    attn_out = low_back(jnp.dot(mixed, w_proj, precision=highest) + proj_bias).reshape(latents, L, D)
    middle = residual + modulation[:, 2] * attn_out
    mlp_input = low(layer_norm(middle) * (1.0 + modulation[:, 4]) + modulation[:, 3]).reshape(latents * L, D)
    upper = low_back(jnp.dot(mlp_input, w_fc1, precision=highest) + fc1_bias)
    hidden = low(jax.nn.gelu(upper, approximate=True))
    mlp_out = low_back(jnp.dot(hidden, w_fc2, precision=highest) + fc2_bias).reshape(latents, L, D)
    return (middle + modulation[:, 5] * mlp_out).reshape(latents * L, D)

def reference(tokens, condition, w_qkv, qv_bias, w_proj, proj_bias, w_fc1, fc1_bias, w_fc2, fc2_bias, w_ada, ada_bias, cotangent):
    params = tuple((param.astype(jnp.float32) for param in (w_qkv, qv_bias, w_proj, proj_bias, w_fc1, fc1_bias, w_fc2, fc2_bias, w_ada, ada_bias)))
    block_seqs = 2 * SEQ_DEV
    blocks = SEQS // block_seqs
    token_blocks = tokens.astype(jnp.float32).reshape(blocks, block_seqs * L, D)
    cond_blocks = condition.astype(jnp.float32).reshape(blocks, block_seqs, D)
    grad_blocks = cotangent.astype(jnp.float32).reshape(blocks, block_seqs * L, D)

    def one_block(totals, item):
        block_tokens, block_cond, block_grad = item
        result, pullback = jax.vjp(forward, block_tokens, block_cond, *params)
        grads = pullback(block_grad)
        updated = tuple((first + second for first, second in zip(totals, grads[2:])))
        return (updated, (result.astype(jnp.bfloat16), grads[0], grads[1]))
    zeros = tuple((jnp.zeros_like(param) for param in params))
    totals, (outputs, grad_tok, grad_cond) = lax.scan(one_block, zeros, (token_blocks, cond_blocks, grad_blocks))
    return (outputs.reshape(TOKENS, D), grad_tok.reshape(TOKENS, D), grad_cond.reshape(SEQS, D), totals[0], totals[1], totals[2], totals[3], totals[4], totals[5], totals[6], totals[7], totals[8], totals[9])
```

```python
from functools import partial
import math

import jax
import jax.numpy as jnp
from jax import lax
from jax.sharding import PartitionSpec as P

HEAD_DIM = 72


eps = 1e-06


def normalize(values):
    center = values - jnp.mean(values, axis=-1, keepdims=True)
    spread = lax.rsqrt(jnp.mean(center * center, axis=-1, keepdims=True) + eps)
    return (center * spread, spread)


def norm_back(gradient, normed, spread):
    return spread * (
        gradient
        - jnp.mean(gradient, axis=-1, keepdims=True)
        - normed * jnp.mean(gradient * normed, axis=-1, keepdims=True)
    )


def contract_last(left_side, right_side):
    return lax.dot_general(
        left_side, right_side, (((1,), (1,)), ((), ())), preferred_element_type=jnp.float32
    )


def contract_first(left_side, right_side):
    return lax.dot_general(
        left_side, right_side, (((0,), (0,)), ((), ())), preferred_element_type=jnp.float32
    )


def gather_rows(values):
    return lax.all_gather(values, "tensor", axis=0, tiled=True)


def gather_grads(values):
    return lax.all_gather(values, "tensor", axis=0, tiled=True)


def sum_rows(source, weight, own_rows):

    def row_term(first_row, number):
        return jnp.dot(source, weight, preferred_element_type=jnp.float32)

    return lax.psum_scatter(
        row_term(jnp.int32(0), lax.axis_size("tensor") * own_rows).astype(jnp.bfloat16),
        "tensor",
        scatter_dimension=0,
        tiled=True,
    ).astype(jnp.float32)


def sum_grads(source, weight, own_rows):

    def row_term(first_row, number):
        return contract_last(source, weight)

    return lax.psum_scatter(
        row_term(jnp.int32(0), lax.axis_size("tensor") * own_rows).astype(jnp.bfloat16),
        "tensor",
        scatter_dimension=0,
        tiled=True,
    ).astype(jnp.float32)


def attend(block):
    query_rows, key_rows, value_rows = block
    scaling = query_rows.shape[-1] ** (-0.5)
    scores = (
        jnp.einsum("sqhe,skhe->shqk", query_rows, key_rows, preferred_element_type=jnp.float32)
        * scaling
    )
    highest = jnp.max(scores, axis=-1, keepdims=True)
    expons = jnp.exp(scores - highest)
    summed = jnp.sum(expons, axis=-1, keepdims=True)
    probs = (expons / summed).astype(jnp.bfloat16)
    mixed = jnp.einsum("shqk,skhe->sqhe", probs, value_rows, preferred_element_type=jnp.float32)
    return (mixed.astype(jnp.bfloat16), (highest + jnp.log(summed))[..., 0])


def attend_back(block):
    query_rows, key_rows, value_rows, logsum, grad_mixed = block
    scaling = query_rows.shape[-1] ** (-0.5)
    scores = (
        jnp.einsum("sqhe,skhe->shqk", query_rows, key_rows, preferred_element_type=jnp.float32)
        * scaling
    )
    probs = jnp.exp(scores - logsum[..., None])
    grad_probs = jnp.einsum(
        "sqhe,skhe->shqk", grad_mixed, value_rows, preferred_element_type=jnp.float32
    )
    grad_values = jnp.einsum(
        "shqk,sqhe->skhe",
        probs.astype(jnp.bfloat16),
        grad_mixed,
        preferred_element_type=jnp.float32,
    )
    grad_scores = (
        probs * (grad_probs - jnp.sum(grad_probs * probs, axis=-1, keepdims=True))
    ).astype(jnp.bfloat16)
    grad_queries = (
        jnp.einsum("shqk,skhe->sqhe", grad_scores, key_rows, preferred_element_type=jnp.float32)
        * scaling
    )
    grad_keys = (
        jnp.einsum("shqk,sqhe->skhe", grad_scores, query_rows, preferred_element_type=jnp.float32)
        * scaling
    )
    return (
        grad_queries.astype(jnp.bfloat16),
        grad_keys.astype(jnp.bfloat16),
        grad_values.astype(jnp.bfloat16),
    )


def per_device(
    tokens,
    condition,
    w_qkv,
    qv_bias,
    w_proj,
    proj_bias,
    w_fc1,
    fc1_bias,
    w_fc2,
    fc2_bias,
    w_ada,
    ada_bias,
    cotangent,
):
    own_rows, width = tokens.shape
    own_seqs = condition.shape[0]
    length = own_rows // own_seqs
    group_rows = own_rows * lax.axis_size("tensor")
    group_seqs = group_rows // length
    local_width = w_qkv.shape[2]
    local_heads = local_width // HEAD_DIM
    block_seqs = math.gcd(group_seqs, max(1, 512 // length))
    blocks = group_seqs // block_seqs
    head_shape = (blocks, block_seqs, length, local_heads, HEAD_DIM)
    cond_float = condition.astype(jnp.float32)
    silu_cond = jax.nn.silu(cond_float).astype(jnp.bfloat16)
    every_cond = lax.all_gather(silu_cond, ("dp", "tensor"), axis=0, tiled=True)
    columns = (
        jnp.dot(every_cond, w_ada, preferred_element_type=jnp.float32)
        + ada_bias.astype(jnp.float32)
    ).astype(jnp.bfloat16)
    modulation = lax.all_to_all(columns, ("dp", "tensor"), split_axis=0, concat_axis=1, tiled=True)
    modul = modulation.astype(jnp.float32).reshape(own_seqs, 6, 1, width)
    shift_attn = modul[:, 0]
    scale_attn = modul[:, 1]
    gate_attn = modul[:, 2]
    shift_mlp = modul[:, 3]
    scale_mlp = modul[:, 4]
    gate_mlp = modul[:, 5]
    qkv_full, proj_full, fc1_full, fc2_full = (
        lax.all_gather(w_qkv, "dp", axis=0, tiled=True),
        lax.all_gather(w_proj, "dp", axis=1, tiled=True),
        lax.all_gather(w_fc1, "dp", axis=0, tiled=True),
        lax.all_gather(w_fc2, "dp", axis=1, tiled=True),
    )
    residual = tokens.astype(jnp.float32).reshape(own_seqs, length, width)
    normed_attn, spread_attn = normalize(residual)
    attn_input = (
        (normed_attn * (1.0 + scale_attn) + shift_attn)
        .astype(jnp.bfloat16)
        .reshape(own_rows, width)
    )
    attn_rows = gather_rows(attn_input)
    projected = jnp.einsum("td,dkf->tkf", attn_rows, qkv_full, preferred_element_type=jnp.float32)
    bias_float = qv_bias.astype(jnp.float32)
    queries = (projected[:, 0] + bias_float[0]).astype(jnp.bfloat16).reshape(head_shape)
    key_all = projected[:, 1].astype(jnp.bfloat16).reshape(head_shape)
    value_all = (projected[:, 2] + bias_float[1]).astype(jnp.bfloat16).reshape(head_shape)
    mixed, logsum = lax.map(attend, (queries, key_all, value_all))
    mixed_rows = mixed.reshape(group_rows, local_width)
    attn_out = (sum_rows(mixed_rows, proj_full, own_rows) + proj_bias.astype(jnp.float32)).reshape(
        own_seqs, length, width
    )
    middle = residual + gate_attn * attn_out
    normed_mlp, spread_mlp = normalize(middle)
    mlp_input = (
        (normed_mlp * (1.0 + scale_mlp) + shift_mlp).astype(jnp.bfloat16).reshape(own_rows, width)
    )
    mlp_rows = gather_rows(mlp_input)
    upper = jnp.dot(mlp_rows, fc1_full, preferred_element_type=jnp.float32) + fc1_bias.astype(
        jnp.float32
    )
    hidden = jax.nn.gelu(upper, approximate=True).astype(jnp.bfloat16)
    mlp_out = (sum_rows(hidden, fc2_full, own_rows) + fc2_bias.astype(jnp.float32)).reshape(
        own_seqs, length, width
    )
    output = (middle + gate_mlp * mlp_out).astype(jnp.bfloat16).reshape(own_rows, width)
    qkv_back, proj_back, fc1_back, fc2_back = (
        lax.all_gather(w_qkv, "dp", axis=0, tiled=True),
        lax.all_gather(w_proj, "dp", axis=1, tiled=True),
        lax.all_gather(w_fc1, "dp", axis=0, tiled=True),
        lax.all_gather(w_fc2, "dp", axis=1, tiled=True),
    )
    grad_out = cotangent.astype(jnp.float32).reshape(own_seqs, length, width)
    grad_mlp = (gate_mlp * grad_out).astype(jnp.bfloat16).reshape(own_rows, width)
    grad_gate_mlp = jnp.sum(grad_out * mlp_out, axis=1)
    grad_mlp_rows = gather_grads(grad_mlp)
    fc2_bias_grad = jnp.sum(grad_mlp_rows.astype(jnp.float32), axis=0)
    fc2_grad = contract_first(hidden, grad_mlp_rows)
    grad_hidden = contract_last(grad_mlp_rows, fc2_back)
    ignored, gelu_pull = jax.vjp(partial(jax.nn.gelu, approximate=True), upper)
    grad_upper = gelu_pull(grad_hidden)[0].astype(jnp.bfloat16)
    fc1_bias_grad = jnp.sum(grad_upper.astype(jnp.float32), axis=0)
    fc1_grad = contract_first(mlp_rows, grad_upper)
    grad_mlp_input = sum_grads(grad_upper, fc1_back, own_rows).reshape(own_seqs, length, width)
    grad_shift_mlp = jnp.sum(grad_mlp_input, axis=1)
    grad_scale_mlp = jnp.sum(grad_mlp_input * normed_mlp, axis=1)
    grad_middle = grad_out + norm_back(grad_mlp_input * (1.0 + scale_mlp), normed_mlp, spread_mlp)
    grad_attn = (gate_attn * grad_middle).astype(jnp.bfloat16).reshape(own_rows, width)
    grad_gate_attn = jnp.sum(grad_middle * attn_out, axis=1)
    grad_attn_rows = gather_grads(grad_attn)
    proj_bias_grad = jnp.sum(grad_attn_rows.astype(jnp.float32), axis=0)
    proj_grad = contract_first(mixed_rows, grad_attn_rows)
    grad_mixed = contract_last(grad_attn_rows, proj_back).astype(jnp.bfloat16).reshape(head_shape)
    grad_query, grad_key, grad_value = lax.map(
        attend_back, (queries, key_all, value_all, logsum, grad_mixed)
    )
    grad_qkv = jnp.stack(
        [
            grad_query.reshape(group_rows, local_width),
            grad_key.reshape(group_rows, local_width),
            grad_value.reshape(group_rows, local_width),
        ],
        axis=1,
    )
    qv_bias_grad = jnp.stack(
        [
            jnp.sum(grad_qkv[:, 0].astype(jnp.float32), axis=0),
            jnp.sum(grad_qkv[:, 2].astype(jnp.float32), axis=0),
        ],
        axis=0,
    )
    qkv_grad = jnp.einsum("td,tkf->dkf", attn_rows, grad_qkv, preferred_element_type=jnp.float32)
    grad_attn_input = sum_grads(
        grad_qkv.reshape(group_rows, 3 * local_width),
        qkv_back.reshape(width, 3 * local_width),
        own_rows,
    ).reshape(own_seqs, length, width)
    grad_shift_attn = jnp.sum(grad_attn_input, axis=1)
    grad_scale_attn = jnp.sum(grad_attn_input * normed_attn, axis=1)
    grad_tokens = (
        grad_middle + norm_back(grad_attn_input * (1.0 + scale_attn), normed_attn, spread_attn)
    ).reshape(own_rows, width)
    grad_modulation = (
        jnp.stack(
            [
                grad_shift_attn,
                grad_scale_attn,
                grad_gate_attn,
                grad_shift_mlp,
                grad_scale_mlp,
                grad_gate_mlp,
            ],
            axis=1,
        )
        .reshape(own_seqs, 6 * width)
        .astype(jnp.bfloat16)
    )
    qkv_grad, proj_grad, fc1_grad, fc2_grad = (
        lax.psum_scatter(qkv_grad.astype(jnp.bfloat16), "dp", scatter_dimension=0, tiled=True).astype(jnp.float32),
        lax.psum_scatter(proj_grad.astype(jnp.bfloat16), "dp", scatter_dimension=1, tiled=True).astype(jnp.float32),
        lax.psum_scatter(fc1_grad.astype(jnp.bfloat16), "dp", scatter_dimension=0, tiled=True).astype(jnp.float32),
        lax.psum_scatter(fc2_grad.astype(jnp.bfloat16), "dp", scatter_dimension=1, tiled=True).astype(jnp.float32),
    )
    qv_bias_grad, proj_bias_grad, fc1_bias_grad, fc2_bias_grad = lax.psum(
        (qv_bias_grad, proj_bias_grad, fc1_bias_grad, fc2_bias_grad), "dp"
    )
    grad_columns = lax.all_to_all(
        grad_modulation, ("dp", "tensor"), split_axis=1, concat_axis=0, tiled=True
    )
    ada_grad = contract_first(every_cond, grad_columns)
    ada_bias_grad = jnp.sum(grad_columns.astype(jnp.float32), axis=0)
    grad_silu = lax.psum_scatter(
        contract_last(grad_columns, w_ada), ("dp", "tensor"), scatter_dimension=0, tiled=True
    )
    ignored_cond, silu_pull = jax.vjp(jax.nn.silu, cond_float)
    grad_condition = silu_pull(grad_silu)[0]
    return (
        output,
        grad_tokens,
        grad_condition,
        qkv_grad,
        qv_bias_grad,
        proj_grad,
        proj_bias_grad,
        fc1_grad,
        fc1_bias_grad,
        fc2_grad,
        fc2_bias_grad,
        ada_grad,
        ada_bias_grad,
    )


def solution(mesh):
    placed = (
        P(("dp", "tensor"), None),
        P(("dp", "tensor"), None),
        P("dp", None, "tensor"),
        P(None, "tensor"),
        P("tensor", "dp"),
        P(),
        P("dp", "tensor"),
        P("tensor"),
        P("tensor", "dp"),
        P(),
        P(None, ("dp", "tensor")),
        P(("dp", "tensor")),
        P(("dp", "tensor"), None),
    )
    return jax.shard_map(
        per_device,
        mesh=mesh,
        in_specs=placed,
        out_specs=(
            P(("dp", "tensor"), None),
            P(("dp", "tensor"), None),
            P(("dp", "tensor"), None),
            P("dp", None, "tensor"),
            P(None, "tensor"),
            P("tensor", "dp"),
            P(),
            P("dp", "tensor"),
            P("tensor"),
            P("tensor", "dp"),
            P(),
            P(None, ("dp", "tensor")),
            P(("dp", "tensor")),
        ),
        check_vma=False,
    )
```
